16 devices in a mesh: col: 2 (over z), row: 8 (over y, x, core).
Axes of the slice: x: 2, y: 2, z: 2, core: 2. Of those that a mesh axis runs over, the one named last changes fastest.
Arguments:
- t_amps: float32 [256, 11664], P('row', 'col')
- denoms: float32 [256, 11664], P('row', 'col')
- v_oovv: bfloat16 [256, 11664], P('row', 'col')
- v_vvvv: bfloat16 [11664, 11664], P('row', 'col')
- v_oooo: bfloat16 [256, 256], replicated
- w_direct: bfloat16 [1728, 1728], P(None, 'col')
- w_exch: bfloat16 [1728, 1728], P(None, 'col')
Outputs:
- output: float32 [256, 11664], P('row', 'col')
All inputs are finite; a program needn't handle non-finite values.
Results may differ from the reference program's by a relative error of at most 0.001.
Values are sent between devices in bfloat16 or wider.
A program may use at most 1 GiB of HBM per device.

```python
import jax
import jax.numpy as jnp

OCC = 16
VIRT = 108
PAIRS_OCC = OCC * OCC
PAIRS_VIRT = VIRT * VIRT
PH_DIM = OCC * VIRT


def setup_inputs(seed: int = 0) -> dict:
    keys = jax.random.split(jax.random.key(seed), 7)
    amp_scale = 1.5 * (OCC * VIRT) ** -0.5
    t_amps = amp_scale * jax.random.normal(keys[0], (PAIRS_OCC, PAIRS_VIRT), jnp.float32)
    denoms = -jax.random.uniform(keys[1], (PAIRS_OCC, PAIRS_VIRT), jnp.float32, 1.0, 3.0)
    v_oovv = jax.random.normal(keys[2], (PAIRS_OCC, PAIRS_VIRT), jnp.float32).astype(jnp.bfloat16)
    vvvv_scale = (OCC / VIRT) ** 0.5 / 1.5
    v_vvvv = (vvvv_scale * jax.random.normal(keys[3], (PAIRS_VIRT, PAIRS_VIRT), jnp.float32)).astype(jnp.bfloat16)
    oooo_scale = (VIRT / OCC) ** 0.5 / 1.5
    v_oooo = (oooo_scale * jax.random.normal(keys[4], (PAIRS_OCC, PAIRS_OCC), jnp.float32)).astype(jnp.bfloat16)
    w_direct = (0.6 * jax.random.normal(keys[5], (PH_DIM, PH_DIM), jnp.float32)).astype(jnp.bfloat16)
    w_exch = (0.6 * jax.random.normal(keys[6], (PH_DIM, PH_DIM), jnp.float32)).astype(jnp.bfloat16)
    return {"t_amps": t_amps, "denoms": denoms, "v_oovv": v_oovv, "v_vvvv": v_vvvv, "v_oooo": v_oooo, "w_direct": w_direct, "w_exch": w_exch}


def reference(t_amps, denoms, v_oovv, v_vvvv, v_oooo, w_direct, w_exch):
    t_half = t_amps.astype(jnp.bfloat16)
    ladder = jnp.dot(t_half, v_vvvv, preferred_element_type=jnp.float32)
    inter_x = jnp.dot(v_oovv, t_half.T, preferred_element_type=jnp.float32)
    hole_mat = (v_oooo.astype(jnp.float32) + 0.5 * inter_x).astype(jnp.bfloat16)
    hole_term = jnp.dot(hole_mat.T, t_half, preferred_element_type=jnp.float32)
    t_wide = t_half.astype(jnp.float32).reshape(OCC, OCC, VIRT, VIRT)
    wd_wide = w_direct.astype(jnp.float32).reshape(OCC, VIRT, OCC, VIRT)
    wx_wide = w_exch.astype(jnp.float32).reshape(OCC, VIRT, OCC, VIRT)
    direct_term = jnp.einsum("ikac,kcjb->ijab", t_wide, wd_wide)
    exch_term = jnp.einsum("ikcb,kcja->ijab", t_wide, wx_wide)
    ph_net = direct_term - exch_term
    ph_sym = (ph_net + ph_net.transpose(1, 0, 3, 2)).reshape(PAIRS_OCC, PAIRS_VIRT)
    residual = v_oovv.astype(jnp.float32) + ladder + hole_term + ph_sym
    return residual / denoms
```

```python
import functools
import jax
import jax.numpy as jnp
from jax import lax
from jax.experimental import pallas as pl
from jax.experimental.pallas import tpu as pltpu
from jax.sharding import PartitionSpec as P

F32 = jnp.float32
BF16 = jnp.bfloat16
OCC = 16
VIRT = 108
NR = 8
HALF = VIRT // 2
CBLK = VIRT * VIRT // NR
COLS = VIRT * VIRT // 2
ROWS = 2 * OCC
CW = 768
NCH = -(-COLS // CW)
LASTW = COLS - (NCH - 1) * CW
HP = 56
VP = 112
VM = pl.BlockSpec(memory_space=pltpu.VMEM)
ANY = pl.BlockSpec(memory_space=pl.ANY)
MESH = pl.DeviceIdType.MESH


def nt_dot(a, b):
    return lax.dot_general(a, b, (((1,), (1,)), ((), ())), preferred_element_type=F32)


def rcopy(src, dst, ssem, rsem, row, col):
    return pltpu.make_async_remote_copy(src_ref=src, dst_ref=dst, send_sem=ssem, recv_sem=rsem,
                                        device_id={"row": row, "col": col}, device_id_type=MESH)


def greet(barrier, row, col):
    pl.semaphore_signal(barrier, inc=1, device_id={"row": row, "col": col}, device_id_type=MESH)


def gather_kernel(t_ref, v_ref, oo_ref, lad, tf, tb, mt, vs, vl, xp, xr, mm,
                  z_s, z_r, l_s, l_r, v_s, v_r, x_s, x_r, m_s, m_r):
    r = lax.axis_index("row")
    c = lax.axis_index("col")
    oc = 1 - c
    barrier = pltpu.get_barrier_semaphore()
    for d in range(1, NR):
        rp = lax.rem(r + d, NR)
        greet(barrier, rp, c)
        greet(barrier, rp, oc)
    greet(barrier, r, oc)

    tb[...] = t_ref[...].astype(BF16)
    for m in range(4):
        tf[4 * c + m] = t_ref[:, m * CBLK:(m + 1) * CBLK].astype(BF16)
        vs[m] = v_ref[:, m * CBLK:(m + 1) * CBLK]
    pl.semaphore_wait(barrier, 2 * NR - 1)

    zc = [rcopy(tf.at[4 * c + m], tf.at[4 * c + m], z_s.at[m], z_r.at[m], r, oc) for m in range(4)]
    for cp in zc:
        cp.start()

    def ladder(rp):
        return rcopy(tf.at[rp], lad.at[r], l_s.at[rp], l_r.at[r], rp, c)

    def send_ladder(rp):
        @pl.when(rp != r)
        def _():
            ladder(rp).start()

        @pl.when(rp == r)
        def _():
            lad[r] = tf[rp]

    for m in range(4):
        send_ladder(4 * c + m)

    def vcopy(m, cp):
        return rcopy(vs.at[m, pl.ds(16 * cp, 16)], vl.at[r], v_s.at[m, cp], v_r.at[r], 4 * c + m, cp)

    for m in range(4):
        for cp in range(2):
            self = jnp.logical_and(4 * c + m == r, c == cp)

            @pl.when(jnp.logical_not(self))
            def _():
                vcopy(m, cp).start()

            @pl.when(self)
            def _():
                vl[r] = vs[m, 16 * cp:16 * cp + 16]

    for m in range(4):
        rcopy(tf.at[4 * oc + m], tf.at[4 * oc + m], z_s.at[m], z_r.at[m], r, oc).wait_recv()
        send_ladder(4 * oc + m)

    for d in range(1, NR):
        s = lax.rem(r + d, NR)
        rcopy(lad.at[s], lad.at[s], l_s.at[s], l_r.at[s], s, c).wait_recv()
    for s in range(NR):
        @pl.when(jnp.logical_not(jnp.logical_and(s == r, c == s // 4)))
        def _():
            rcopy(vl.at[s], vl.at[s], v_s.at[0, 0], v_r.at[s], s, c).wait_recv()

    xp[...] = nt_dot(vl[...].reshape(NR * 16, CBLK), lad[...].reshape(NR * ROWS, CBLK)).reshape(NR, 16, NR * ROWS)

    def xcopy(s):
        return rcopy(xp.at[s], xr.at[r], x_s.at[s], x_r.at[r], s, c)

    for d in range(1, NR):
        xcopy(lax.rem(r + d, NR)).start()
    xr[r] = xp[r]
    for d in range(1, NR):
        s = lax.rem(r + d, NR)
        rcopy(xr.at[s], xr.at[s], x_s.at[s], x_r.at[s], s, c).wait_recv()
    xsum = xr[0]
    for s in range(1, NR):
        xsum = xsum + xr[s]
    oo = oo_ref[pl.ds(pl.multiple_of(ROWS * r + 16 * c, 16), 16), :]
    mm[c] = (oo.astype(F32) + 0.5 * xsum).astype(BF16)
    mcp = rcopy(mm.at[c], mm.at[c], m_s, m_r, r, oc)
    mcp.start()
    rcopy(mm.at[oc], mm.at[oc], m_s, m_r, r, oc).wait_recv()
    mt[...] = mm[...].reshape(ROWS, NR * ROWS).astype(F32).T.astype(BF16)

    mcp.wait_send()
    for cp in zc:
        cp.wait_send()
    for d in range(1, NR):
        s = lax.rem(r + d, NR)
        ladder(s).wait_send()
        xcopy(s).wait_send()
    for m in range(4):
        for cp in range(2):
            @pl.when(jnp.logical_not(jnp.logical_and(4 * c + m == r, c == cp)))
            def _():
                vcopy(m, cp).wait_send()


def gather_call(t_blk, v_blk, oooo):
    dma = pltpu.SemaphoreType.DMA
    return pl.pallas_call(
        gather_kernel,
        name="gather",
        out_shape=(
            jax.ShapeDtypeStruct((NR, ROWS, CBLK), BF16),
            jax.ShapeDtypeStruct((NR, ROWS, CBLK), BF16),
            jax.ShapeDtypeStruct((ROWS, COLS), BF16),
            jax.ShapeDtypeStruct((NR * ROWS, ROWS), BF16),
        ),
        in_specs=[VM] * 3,
        out_specs=(VM,) * 4,
        scratch_shapes=[
            pltpu.VMEM((4, ROWS, CBLK), BF16),
            pltpu.VMEM((NR, 16, CBLK), BF16),
            pltpu.VMEM((NR, 16, NR * ROWS), F32),
            pltpu.VMEM((NR, 16, NR * ROWS), F32),
            pltpu.VMEM((2, 16, NR * ROWS), BF16),
            dma((4,)), dma((4,)), dma((NR,)), dma((NR,)), dma((4, 2)), dma((NR,)),
            dma((NR,)), dma((NR,)), dma, dma,
        ],
        compiler_params=pltpu.CompilerParams(collective_id=0, has_side_effects=True),
        cost_estimate=pl.CostEstimate(flops=2 * 128 * 256 * CBLK, bytes_accessed=4 * 10**6, transcendentals=0),
    )(t_blk, v_blk, oooo)


def ph_kernel(tf, wd, wx, so, sto, rr, td, te, dd, ff):
    for a in range(VIRT):
        p = a * VIRT
        b, off = p // CBLK, p % CBLK
        n1 = min(VIRT, CBLK - off)
        rr[a * ROWS:(a + 1) * ROWS, 0:n1] = tf[b, :, off:off + n1].astype(F32)
        if n1 < VIRT:
            rr[a * ROWS:(a + 1) * ROWS, n1:VIRT] = tf[b + 1, :, 0:VIRT - n1].astype(F32)
    for i in range(2):
        for k in range(OCC):
            blk = rr[pl.ds(i * OCC + k, 128, stride=ROWS), :]
            td[i * VP:i * VP + VIRT, k * VIRT:(k + 1) * VIRT] = blk[:VIRT, :VIRT].astype(BF16)
            te[i * VP:i * VP + VIRT, k * VIRT:(k + 1) * VIRT] = blk.T[:VIRT, :VIRT].astype(BF16)
    dd[...] = jnp.dot(td[...], wd[...], preferred_element_type=F32)
    ff[...] = jnp.dot(te[...], wx[...], preferred_element_type=F32)
    for j in range(OCC // 2):
        for i in range(2):
            d_ij = dd[i * VP:i * VP + VP, j * VIRT:(j + 1) * VIRT]
            f_ij = ff[i * VP:i * VP + VP, j * VIRT:(j + 1) * VIRT]
            s = d_ij[:VIRT, :VIRT] - f_ij.T[:VIRT, :VIRT]
            st = d_ij.T[:VIRT, :VIRT] - f_ij[:VIRT, :VIRT]
            for h in range(2):
                so[h, j, i, 0:HALF, 0:VIRT] = s[h * HALF:(h + 1) * HALF]
                sto[h, j // 2, 2 * (j % 2) + i, 0:HALF, 0:VIRT] = st[h * HALF:(h + 1) * HALF]


def ph_call(tf, wd, wx):
    ncol = wd.shape[1]
    return pl.pallas_call(
        ph_kernel,
        name="ph",
        out_shape=(
            jax.ShapeDtypeStruct((2, 8, 2, HP, 128), F32),
            jax.ShapeDtypeStruct((2, 4, 4, HP, 128), F32),
        ),
        in_specs=[VM] * 3,
        out_specs=(VM,) * 2,
        scratch_shapes=[
            pltpu.VMEM((128 * ROWS, 128), F32),
            pltpu.VMEM((2 * VP, OCC * VIRT), BF16),
            pltpu.VMEM((2 * VP, OCC * VIRT), BF16),
            pltpu.VMEM((2 * VP, ncol), F32),
            pltpu.VMEM((2 * VP, ncol), F32),
        ],
        cost_estimate=pl.CostEstimate(flops=4 * 224 * 1728 * 864, bytes_accessed=8 * 10**6, transcendentals=0),
    )(tf, wd, wx)


def ladder_kernel(lad, mt, tb, so, sto, v_hbm, rs, sz, strr, vbuf, part, d2d, r1, r2, stz,
                  v_sem, d_s, d_r, a_s, a_r, b_s, b_r, s_s, s_r, t_s, t_r):
    row = lax.axis_index("row")
    c = lax.axis_index("col")
    oc = 1 - c
    core = lax.rem(row, 2)
    q = row // 2
    x, y = lax.rem(q, 2), q // 2
    qs = {"x": 2 * y + 1 - x, "y": 2 * (1 - y) + x, "d": 2 * (1 - y) + 1 - x}
    barrier = pltpu.get_barrier_semaphore()
    for d in range(1, NR):
        greet(barrier, lax.rem(row + d, NR), c)
    greet(barrier, row, oc)

    v_copy = pltpu.make_async_copy(v_hbm, vbuf, v_sem)
    v_copy.start()
    pl.semaphore_wait(barrier, NR)

    stz_cp = rcopy(sto.at[oc], stz, s_s.at[0], s_r.at[0], row, oc)
    sz_cp = rcopy(so.at[oc], sz, s_s.at[1], s_r.at[1], row, oc)
    stz_cp.start()
    sz_cp.start()

    def tcopy(jr, own):
        rp = 4 * c + jr if own else 4 * oc + jr
        src = sto.at[c, jr] if own else stz.at[jr]
        return rp, rcopy(src, strr.at[row], t_s.at[rp], t_r.at[row], rp, c)

    def send_t(jr, own):
        rp, cp = tcopy(jr, own)

        @pl.when(rp != row)
        def _():
            cp.start()

        @pl.when(rp == row)
        def _():
            strr[row] = sto[c, jr] if own else stz[jr]

    for jr in range(4):
        send_t(jr, True)

    def d_copy(n):
        return rcopy(part.at[n, :, 1 - core], d2d.at[n], d_s.at[n], d_r.at[n], 2 * q + 1 - core, c)

    XR = pl.ds(0, 16)
    YR = pl.ds(16, 16)

    def a_copies(n):
        out = []
        for e, (nb, far, rows) in enumerate((("x", "x", XR), ("x", "d", XR), ("y", "y", YR), ("y", "d", YR))):
            out.append(rcopy(part.at[n, qs[far], core, rows], r1.at[n, e], a_s.at[n, e], a_r.at[n, e],
                             2 * qs[nb] + core, c))
        return out

    def b_copies(n):
        return [rcopy(part.at[n, qs["y"], core, XR], r2.at[n, 0], b_s.at[n, 0], b_r.at[n, 0], 2 * qs["y"] + core, c),
                rcopy(part.at[n, qs["x"], core, YR], r2.at[n, 1], b_s.at[n, 1], b_r.at[n, 1], 2 * qs["x"] + core, c)]

    def compute(n):
        w = CW if n < NCH - 1 else LASTW
        p = jnp.dot(lad[...], vbuf[:, n * CW:n * CW + w], preferred_element_type=F32)
        p = p + jnp.dot(mt[...], tb[:, n * CW:n * CW + w], preferred_element_type=F32)
        part[n, :, :, :, 0:w] = p.reshape(4, 2, ROWS, w)
        d_copy(n).start()

    def first(n):
        d_copy(n).wait_recv()
        for k in range(4):
            part[n, k, core] = part[n, k, core] + d2d[n, k]
        for cp in a_copies(n):
            cp.start()

    v_copy.wait()
    for n in range(NCH):
        compute(n)
        if n >= 1:
            first(n - 1)
    first(NCH - 1)

    rcopy(stz, stz, s_s.at[0], s_r.at[0], row, oc).wait_recv()
    for jr in range(4):
        send_t(jr, False)

    def second(n):
        for cp in a_copies(n):
            cp.wait_recv()
        part[n, qs["y"], core, 0:16] = part[n, qs["y"], core, 0:16] + r1[n, 1]
        part[n, qs["x"], core, 16:32] = part[n, qs["x"], core, 16:32] + r1[n, 3]
        for cp in b_copies(n):
            cp.start()

    for n in range(NCH):
        second(n)

    def third(n):
        for cp in b_copies(n):
            cp.wait_recv()
        rs[n, 0:16] = part[n, q, core, 0:16] + r1[n, 0] + r2[n, 0]
        rs[n, 16:32] = part[n, q, core, 16:32] + r1[n, 2] + r2[n, 1]

    for n in range(NCH):
        third(n)

    rcopy(sz, sz, s_s.at[1], s_r.at[1], row, oc).wait_recv()
    for d in range(1, NR):
        s = lax.rem(row + d, NR)
        rcopy(strr.at[s], strr.at[s], t_s.at[s], t_r.at[s], s, c).wait_recv()
    stz_cp.wait_send()
    sz_cp.wait_send()
    for d in range(1, NR):
        s = lax.rem(row + d, NR)
        rcopy(strr.at[s], strr.at[s], t_s.at[s], t_r.at[s], s, c).wait_send()
    for n in range(NCH):
        d_copy(n).wait_send()
        for cp in a_copies(n) + b_copies(n):
            cp.wait_send()


def ladder_call(lad, mt, tb, so, sto, vvvv):
    dma = pltpu.SemaphoreType.DMA
    return pl.pallas_call(
        ladder_kernel,
        name="ladder",
        out_shape=(
            jax.ShapeDtypeStruct((NCH, ROWS, CW), F32),
            jax.ShapeDtypeStruct((8, 2, HP, 128), F32),
            jax.ShapeDtypeStruct((NR, 4, HP, 128), F32),
        ),
        in_specs=[VM] * 5 + [ANY],
        out_specs=(VM,) * 3,
        scratch_shapes=[
            pltpu.VMEM((CBLK, COLS), BF16),
            pltpu.VMEM((NCH, 4, 2, ROWS, CW), F32),
            pltpu.VMEM((NCH, 4, ROWS, CW), F32),
            pltpu.VMEM((NCH, 4, 16, CW), F32),
            pltpu.VMEM((NCH, 2, 16, CW), F32),
            pltpu.VMEM((4, 4, HP, 128), F32),
            dma, dma((NCH,)), dma((NCH,)), dma((NCH, 4)), dma((NCH, 4)), dma((NCH, 2)), dma((NCH, 2)),
            dma((2,)), dma((2,)), dma((NR,)), dma((NR,)),
        ],
        compiler_params=pltpu.CompilerParams(collective_id=1, has_side_effects=True, vmem_limit_bytes=60 * 2**20),
        cost_estimate=pl.CostEstimate(flops=2 * 256 * CBLK * COLS, bytes_accessed=20 * 10**6, transcendentals=0),
    )(lad, mt, tb, so, sto, vvvv)


def final_kernel(rs, v_ref, d_ref, so, sz, strr, out, rr, zz):
    c = lax.axis_index("col")
    oc = 1 - c
    for i in range(2):
        for jj in range(8):
            for mine in range(2):
                h = c if mine else oc
                blk = so[c, jj, i, 0:HALF] if mine else sz[jj, i, 0:HALF]
                blk = blk + strr[4 * h + jj // 2, 2 * i + jj % 2, 0:HALF]
                rr[pl.ds(i * OCC + 8 * h + jj, HALF, stride=ROWS), :] = blk
    for a in range(HALF):
        zz[:, a * VIRT:(a + 1) * VIRT] = rr[a * ROWS:(a + 1) * ROWS, 0:VIRT]
    for n in range(NCH):
        w = CW if n < NCH - 1 else LASTW
        sl = slice(n * CW, n * CW + w)
        out[:, sl] = (v_ref[:, sl].astype(F32) + rs[n, :, 0:w] + zz[:, sl]) / d_ref[:, sl]


def final_call(rs, v_blk, d_blk, so, sz, strr):
    return pl.pallas_call(
        final_kernel,
        name="final",
        out_shape=jax.ShapeDtypeStruct((ROWS, COLS), F32),
        in_specs=[VM] * 6,
        out_specs=VM,
        scratch_shapes=[pltpu.VMEM((HALF * ROWS, 128), F32), pltpu.VMEM((ROWS, COLS), F32)],
        cost_estimate=pl.CostEstimate(flops=10**6, bytes_accessed=4 * 10**6, transcendentals=0),
    )(rs, v_blk, d_blk, so, sz, strr)


def solution(mesh):
    amp_spec = P("row", "col")
    wide_spec = P(None, "col")

    def local_sweep(t_blk, d_blk, oovv_blk, vvvv_blk, oooo_full, wd_blk, wx_blk):
        lad, tf, tb, mt = gather_call(t_blk, oovv_blk, oooo_full)
        so, sto = ph_call(tf, wd_blk, wx_blk)
        rs, sz, strr = ladder_call(lad.reshape(NR * ROWS, CBLK), mt, tb, so, sto, vvvv_blk)
        return final_call(rs, oovv_blk, d_blk, so, sz, strr)

    return jax.shard_map(local_sweep, mesh=mesh, in_specs=(amp_spec, amp_spec, amp_spec, amp_spec, P(), wide_spec, wide_spec), out_specs=amp_spec, check_vma=False)
```
